32 devices in a mesh: replica: 4 (over x, core), fsdp: 4 (over z), tensor: 2 (over y).
Axes of the slice: x: 2, y: 2, z: 4, core: 2. Of those that a mesh axis runs over, the one named last changes fastest.
Arguments:
- pseudo_grad: bfloat16 [4, 3072, 18432], P('replica', 'fsdp', 'tensor'), may hold values from -6 to 6
- compensation: float32 [4, 3072, 18432], P('replica', 'fsdp', 'tensor'), may hold values from -6 to 6
- params: float32 [3072, 18432], P(('fsdp', 'replica'), 'tensor'), may hold values from -6 to 6
- momentum: float32 [3072, 18432], P(('fsdp', 'replica'), 'tensor'), may hold values from -6 to 6
- probe: bfloat16 [256, 18432], P('fsdp', 'tensor'), may hold values from -0.046875 to 0.046875
Outputs:
- new_params: float32 [3072, 18432], P(('fsdp', 'replica'), 'tensor')
- new_momentum: float32 [3072, 18432], P(('fsdp', 'replica'), 'tensor')
- probe_out: bfloat16 [256, 3072], P('tensor', 'fsdp')
The draws below stay inside these ranges and needn't reach their ends.
All inputs are finite; a program needn't handle non-finite values.
Results may differ from the reference program's by a relative error of at most 0.014.
Values may be sent and summed in bfloat16 or wider, within the bound.
A program may use at most 128 MiB of HBM per device.

```python
import jax
import jax.numpy as jnp
from jax import lax

D = 3072
FW = 18432
PROBE = 256
N_REPLICA = 4


def spiked(entries, rng, source, target, shards_of, factor):
    def block_of(dim):
        return (jnp.arange(entries.shape[dim]) // (entries.shape[dim] // shards_of)).reshape((-1,) + (1,) * (entries.ndim - 1 - dim))

    one_side = jax.random.permutation(rng, shards_of)[block_of(target)]
    far = (block_of(target) + shards_of // 2) % shards_of
    return jnp.where((block_of(source) == one_side) | (block_of(source) == far), factor * entries, entries)


def steps_of(rng, dims, pieces, smallest, top_value):
    def one(position, parts):
        draws = jax.random.uniform(jax.random.fold_in(jax.random.fold_in(rng, 6), position), (parts,), jnp.float32, smallest / len(pieces), top_value / len(pieces))
        return jnp.repeat(jnp.exp(draws), dims[position] // parts).reshape((-1,) + (1,) * (len(dims) - position - 1))

    factor_of = one(*pieces[0])
    for cut in pieces[1:]:
        factor_of = factor_of * one(*cut)
    return factor_of


def noise(own_key, extent, spread, bound, shards=(), held_as=jnp.bfloat16):
    drawn = spread * jax.random.normal(own_key, extent, jnp.float32)
    if shards:
        drawn = drawn * steps_of(own_key, extent, shards, -0.22, 0.18)
    return jnp.clip(drawn, -bound, bound).astype(held_as)


def heavy_noise(rng, dims, scale, most, shards, heavy, dtype=jnp.bfloat16):
    result = scale * jax.random.normal(rng, dims, jnp.float32)
    if shards:
        result = result * steps_of(rng, dims, shards, -0.22, 0.18)
    return jnp.clip(spiked(result, jax.random.fold_in(rng, 3), *heavy), -most, most).astype(dtype)


def setup_inputs(seed: int = 0) -> dict:
    key_list = jax.random.split(jax.random.key(seed), 6)
    pseudo_grad = heavy_noise(key_list[0], (N_REPLICA, D, FW), 1.0, 6.0, ((0, 4), (1, 4), (2, 2)), (0, 1, 4, 2.0))
    compensation = noise(key_list[1], (N_REPLICA, D, FW), 1.0, 6.0, ((0, 4), (1, 4), (2, 2)), jnp.float32)
    params = noise(key_list[2], (D, FW), 1.0, 6.0, ((0, 16), (1, 2)), jnp.float32)
    momentum = noise(key_list[3], (D, FW), 1.0, 6.0, ((0, 16), (1, 2)), jnp.float32)
    probe = noise(key_list[4], (PROBE, FW), FW ** -0.5, 0.046875, ((0, 4), (1, 2)))
    return dict(pseudo_grad=pseudo_grad, compensation=compensation, params=params, momentum=momentum, probe=probe)


outer_rate = 0.7
nesterov = 0.9


def reference(pseudo_grad, compensation, params, momentum, probe):
    def accumulate(summed, pair):
        grads, carried = pair
        outgoing = (grads.astype(jnp.float32) + carried).astype(jnp.bfloat16)
        outgoing = lax.optimization_barrier(outgoing)
        return summed + outgoing.astype(jnp.float32), None

    start = jnp.zeros(params.shape, jnp.float32)
    summed, _ = lax.scan(accumulate, start, (pseudo_grad, compensation))
    average = summed / N_REPLICA
    new_momentum = nesterov * momentum + average
    new_params = params - outer_rate * (average + nesterov * new_momentum)
    weights = new_params.astype(jnp.bfloat16)
    probe_out = lax.dot_general(probe, weights, (((1,), (1,)), ((), ())), preferred_element_type=jnp.float32)
    return new_params, new_momentum, probe_out.astype(jnp.bfloat16)
```

```python
import functools

import jax
import jax.numpy as jnp
from jax import lax
from jax.experimental import pallas as pl
from jax.experimental.pallas import tpu as pltpu
from jax.sharding import PartitionSpec as P


outer_rate = 0.7
nesterov = 0.9
f32, bf16 = jnp.float32, jnp.bfloat16


def chunk_edges(tiles):
    edges = [0]
    for share in (2 / 18, 6 / 18, 12 / 18, 16 / 18):
        edge = max(1, round(share * tiles))
        if edges[-1] < edge < tiles:
            edges.append(edge)
    return edges + [tiles]


def add_product(offsets, probes, weights, total):
    rows = jnp.concatenate([block[...] for block in probes], axis=0)
    product = lax.dot_general(
        rows, weights, (((1,), (1,)), ((), ())), preferred_element_type=f32
    )
    start = 0
    for i, block in enumerate(probes):
        height = block.shape[0]
        at = pl.ds(pl.multiple_of(offsets[1 + i], height), height)
        total[at, :] += product[start : start + height]
        start += height


def update_kernel(n_replica, n_arrived, n_probe, first, offsets, *refs):
    refs = list(refs)
    take = lambda n: [refs.pop(0) for _ in range(n)]
    grad, carried, params, momentum, mate = take(5)
    arrived = take(n_arrived)
    probes = take(n_probe)
    if not first:
        take(2)
    if n_probe:
        (before,) = take(1)
    elif not first:
        take(1)
    new_params, new_momentum, last = refs

    summed = grad[...].astype(f32) + carried[...] + mate[...].astype(f32)
    for part in arrived:
        summed += part[...].astype(f32)
    average = summed / n_replica
    moved = nesterov * momentum[...] + average
    updated = params[...] - outer_rate * (average + nesterov * moved)
    new_momentum[...] = moved
    new_params[...] = updated
    weights = updated.astype(bf16)
    if not n_probe:
        last[...] = weights
        return

    @pl.when(pl.program_id(0) == 0)
    def _():
        last[...] = before[...]

    add_product(offsets, probes, weights, last)


def product_kernel(offsets, *refs):
    *probes, weights, total = refs

    @pl.when(pl.program_id(0) == 0)
    def _():
        total[...] = jnp.zeros_like(total)

    add_product(offsets, probes, weights[...], total)


def call(kernel, offsets, steps, in_specs, args, out_specs, out_shape, aliases, area, n_rows, wide):
    return pl.pallas_call(
        kernel,
        grid_spec=pltpu.PrefetchScalarGridSpec(
            num_scalar_prefetch=1, grid=(steps,), in_specs=in_specs, out_specs=out_specs
        ),
        out_shape=out_shape,
        input_output_aliases=aliases,
        cost_estimate=pl.CostEstimate(
            flops=2 * area * n_rows, bytes_accessed=wide * area, transcendentals=0
        ),
        compiler_params=pltpu.CompilerParams(dimension_semantics=("arbitrary",)),
    )(offsets, *args)


def update(offsets, lo, hi, tile, n_replica, grad, carried, params, momentum, mate, arrived, probes, state, total):
    rows, columns = params.shape
    if lo % 2 == 0 and hi % 2 == 0 and not probes:
        lo, hi, tile = lo // 2, hi // 2, tile * 2
    there = pl.BlockSpec((rows, tile), lambda j, s: (0, lo + j))
    shard = pl.BlockSpec((None, rows, tile), lambda j, s: (0, s[0], lo + j))
    in_specs = [shard, shard, there, there, there]
    in_specs += [pl.BlockSpec((rows, tile), lambda j, s: (0, j))] * len(arrived)
    in_specs += [pl.BlockSpec((p.shape[0], tile), lambda j, s: (0, lo + j)) for p in probes]
    args = [grad, carried, params, momentum, mate, *arrived, *probes]
    hbm = pl.BlockSpec(memory_space=pl.ANY)
    aliases = {}
    if state is not None:
        kept = state[:2] if probes else state
        aliases = {1 + len(args) + i: i for i in range(len(kept))}
        in_specs += [hbm] * len(kept)
        args += kept
    full = jax.ShapeDtypeStruct((rows, columns), f32)
    n_rows = 0
    if probes:
        n_rows = total.shape[0]
        whole = pl.BlockSpec(total.shape, lambda j, s: (0, 0))
        in_specs.append(whole)
        args.append(total)
        last, last_shape = whole, jax.ShapeDtypeStruct(total.shape, f32)
    else:
        last, last_shape = there, jax.ShapeDtypeStruct((rows, columns), bf16)
    return call(
        functools.partial(update_kernel, n_replica, len(arrived), len(probes), state is None),
        offsets, hi - lo, in_specs, args, [there, there, last], [full, full, last_shape],
        aliases, rows * (hi - lo) * tile, n_rows, 26,
    )


def product(offsets, hi, tile, probes, weights):
    rows, _ = weights.shape
    n_rows = sum(p.shape[0] for p in probes)
    if hi % 2 == 0:
        hi, tile = hi // 2, tile * 2
    at = lambda j, s: (0, j)
    in_specs = [pl.BlockSpec((p.shape[0], tile), at) for p in probes]
    in_specs.append(pl.BlockSpec((rows, tile), at))
    return call(
        product_kernel, offsets, hi, in_specs, [*probes, weights],
        pl.BlockSpec((n_rows, rows), lambda j, s: (0, 0)),
        jax.ShapeDtypeStruct((n_rows, rows), f32), {}, rows * hi * tile, n_rows, 4,
    )


def start_gather(probe, core):
    n = lax.axis_size("fsdp")
    if n > 4:
        return [lax.all_gather(probe, "fsdp", axis=0, tiled=True)]
    half = probe.shape[0] // 2
    mine = lax.dynamic_slice_in_dim(probe, core * half, half, 0)
    return [
        lax.ppermute(mine, "fsdp", [(i, (i + step) % n) for i in range(n)])
        for step in range(1, n)
    ]


def end_gather(probe, fetched, core, partner):
    n = lax.axis_size("fsdp")
    if n > 4:
        return fetched, [jnp.int32(0)]
    here = lax.axis_index("fsdp")
    height = probe.shape[0]
    half = height // 2
    blocks, places = [probe], [here * height]
    for step, block in enumerate(fetched, 1):
        start = (here - step) % n * height
        blocks += [block, lax.ppermute(block, "replica", partner)]
        places += [start + core * half, start + (1 - core) * half]
    return blocks, places


def per_device(pseudo_grad, compensation, params, momentum, probe):
    n = lax.axis_size("replica")
    chips = n // 2
    me = lax.axis_index("replica")
    chip, core = me // 2, me % 2
    rows, columns = params.shape
    tile = 512 if columns % 512 == 0 else 128
    edges = chunk_edges(columns // tile)
    partner = [(i, i ^ 1) for i in range(n)]

    def outgoing(dest, lo, hi):
        where, size = (0, dest * rows, lo * tile), (1, rows, (hi - lo) * tile)
        grads = lax.dynamic_slice(pseudo_grad, where, size)[0]
        return grads.astype(f32) + lax.dynamic_slice(compensation, where, size)[0]

    order = me * 0

    def after(value):
        nonlocal order
        order, value = lax.optimization_barrier((order, value))
        return value

    spans = list(zip(edges, edges[1:]))

    def swap(i):
        lo, hi = spans[i]
        swapped = []
        for step in range(1, chips):
            there = (chip + step) % chips + order
            give = after(outgoing(there * 2 + 1 - core, lo, hi).astype(bf16))
            swapped.append(lax.ppermute(give, "replica", partner))
        return swapped

    def cross(i, swapped):
        lo, hi = spans[i]
        received = []
        for step, got in zip(range(1, chips), swapped):
            there = (chip + step) % chips + order
            part = outgoing(there * 2 + core, lo, hi) + got.astype(f32)
            part = after(part.astype(bf16))
            across = [(i, (i // 2 + step) % chips * 2 + i % 2) for i in range(n)]
            received.append(lax.ppermute(part, "replica", across))
        return received

    arrived = []
    swapped = swap(0)
    for i in range(len(spans)):
        following = swap(i + 1) if i + 1 < len(spans) else None
        arrived.append(cross(i, swapped))
        swapped = following
        if i == 0:
            fetched = start_gather(after(probe), core)
    own = (chip + order) * 2 + 1 - core
    give = after(outgoing(own, 0, edges[-1]).astype(bf16))
    mate = lax.ppermute(give, "replica", partner)
    blocks, places = end_gather(probe, fetched, core, partner)

    offsets = jnp.stack([me + order] + places).astype(jnp.int32)
    fused = len(spans) - 2
    state = total = None
    for i, ((lo, hi), received) in enumerate(zip(spans, arrived)):
        if i == fused:
            total = product(offsets, lo, tile, blocks, state[2])
        state = update(
            offsets, lo, hi, tile, n, pseudo_grad, compensation, params, momentum,
            mate, received, blocks if i >= fused else [], state, total,
        )
        if i >= fused:
            total = state[2]
    new_params, new_momentum, total = state

    splits = lax.axis_size("tensor")
    mine = lax.axis_index("tensor")
    height = total.shape[0] // splits
    piece = lambda which: lax.dynamic_slice_in_dim(total, which * height, height, 0)
    column_part = piece(mine)
    for step in range(1, splits):
        shift = [(i, (i + step) % splits) for i in range(splits)]
        sent = piece((mine + step) % splits).astype(bf16)
        column_part += lax.ppermute(sent, "tensor", shift).astype(f32)
    probe_out = lax.all_gather(column_part.astype(bf16), "replica", axis=1, tiled=True)
    return (new_params, new_momentum, probe_out)


def solution(mesh):
    in_specs = (
        P("replica", "fsdp", "tensor"),
        P("replica", "fsdp", "tensor"),
        P(("fsdp", "replica"), "tensor"),
        P(("fsdp", "replica"), "tensor"),
        P("fsdp", "tensor"),
    )
    out_specs = (
        P(("fsdp", "replica"), "tensor"),
        P(("fsdp", "replica"), "tensor"),
        P("tensor", "fsdp"),
    )

    return jax.shard_map(
        per_device, mesh=mesh, in_specs=in_specs, out_specs=out_specs, check_vma=False
    )
```
